32 devices in a mesh: slab: 8 (over z, y), sub: 4 (over x, core).
Axes of the slice: x: 2, y: 2, z: 4, core: 2. Of those that a mesh axis runs over, the one named last changes fastest.
Arguments:
- factor_obs: float32 [32, 64, 64, 512], P('slab', 'sub'), may hold values from -0.20992233 to 0.20992233
- factor_ctrl: float32 [32, 64, 64, 512], P('slab', 'sub'), may hold values from -0.20992233 to 0.20992233
- diffusivity: float32 [32, 4096], P('slab', 'sub'), may hold values from 0.5 to 2
- input_map: float32 [4, 32, 4096], P(None, 'slab', 'sub'), may hold values from -2 to 2
- output_map: float32 [4, 32, 4096], P(None, 'slab', 'sub'), may hold values from -2 to 2
- start_block: float32 [512, 128], replicated, may hold values from -6 to 6
- order: int32 [1], replicated, may hold values from 64 to 128
Outputs:
- reduced_mass: float32 [128, 128], replicated
- reduced_state: float32 [128, 128], replicated
- reduced_input: float32 [128, 4], replicated
- reduced_output: float32 [4, 128], replicated
The draws below stay inside these ranges and needn't reach their ends.
All inputs are finite; a program needn't handle non-finite values.
Results may differ from the reference program's by a relative error of at most 0.00017.
Values sent between devices are 32-bit elements; how exact they have to be, the bound alone decides.
A program may use at most 128 MiB of HBM per device.

```python
import math
import jax
import jax.numpy as jnp
from jax import lax

NX = 64
RANK = 512
RMAX = 128
NIN = 4
NOUT = 4
POWER = 2
NZ = 32
NY = 64
NYX = 4096
NCELL = 131072


def factor_draw(key, salt):
    key = jax.random.fold_in(key, salt)
    entry_key, level_key = jax.random.split(key)
    entries = jnp.clip(jax.random.normal(entry_key, (NZ, NY, NX, RANK), jnp.float32), -6.0, 6.0)
    level = jax.random.uniform(level_key, (NZ, NY, NX), jnp.float32) * math.log(10.0)
    rising = 1.0 + 2.0 * jnp.arange(NZ, dtype=jnp.float32) / max(NZ - 1, 1)
    scales = jnp.exp(level) * rising[:, None, None] / 9.65 * float(NCELL * RANK) ** (-0.25)
    return (entries * scales[..., None]).astype(jnp.float32)


def draw_factor_obs(key, part):
    return factor_draw(key, 11)


def draw_factor_ctrl(key, part):
    return factor_draw(key, 23)


def block_levels(rng, dims, pieces, smallest, high):
    def one(dim, parts):
        heights = jax.random.uniform(jax.random.fold_in(jax.random.fold_in(rng, 6), dim), (parts,), jnp.float32, smallest / len(pieces), high / len(pieces))
        return jnp.repeat(jnp.exp(heights), dims[dim] // parts).reshape((-1,) + (1,) * (len(dims) - dim - 1))

    level = one(*pieces[0])
    for cut in pieces[1:]:
        level = level * one(*cut)
    return level


def centred(rng, shape, spread, limit, cuts=(), kind=jnp.bfloat16):
    values = spread * jax.random.normal(rng, shape, jnp.float32)
    if cuts:
        values = values * block_levels(rng, shape, cuts, -0.22, 0.18)
    return jnp.clip(values, -limit, limit).astype(kind)


def setup_inputs(seed: int = 0) -> dict:
    key_list = jax.random.split(jax.random.key(seed), 8)
    factor_obs = draw_factor_obs(jax.random.fold_in(key_list[7], 71), 0)
    factor_ctrl = draw_factor_ctrl(jax.random.fold_in(key_list[7], 71), 0)
    diffusivity = jnp.clip(jnp.exp(math.log(2.0) - 1.3862944 * jax.random.uniform(key_list[2], (NZ, NYX), jnp.float32) ** block_levels(key_list[2], (NZ, NYX), ((0, 8), (1, 4)), -0.2, 0.2)), 0.5, 2.0)
    input_map = centred(key_list[3], (NIN, NZ, NYX), (max(NCELL // RANK // 32, 1)) ** -0.5, 2.0, ((1, 8), (2, 4)), jnp.float32)
    output_map = centred(key_list[4], (NOUT, NZ, NYX), (max(NCELL // RANK // 32, 1)) ** -0.5, 2.0, ((1, 8), (2, 4)), jnp.float32)
    start_block = centred(key_list[5], (RANK, RMAX), 1.0, 6.0, (), jnp.float32)
    order = jax.random.randint(key_list[6], (1,), RMAX // 2, RMAX + 1).astype(jnp.int32)
    return dict(factor_obs=factor_obs, factor_ctrl=factor_ctrl, diffusivity=diffusivity, input_map=input_map, output_map=output_map, start_block=start_block, order=order)


def matmul(first, second):
    return jnp.dot(first.astype(jnp.float32), second.astype(jnp.float32), precision=lax.Precision.HIGHEST, preferred_element_type=jnp.float32)

def orthonormal(start):
    gram = matmul(start.T, start)
    lower_factor = jnp.linalg.cholesky(gram)
    return lax.linalg.triangular_solve(lower_factor, start, left_side=False, lower=True, transpose_a=True)

def subspace_bases(cross_gram, start_block):
    right_basis = orthonormal(matmul(cross_gram.T, start_block))
    left_basis = orthonormal(matmul(cross_gram, right_basis))
    for repeat in range(POWER - 1):
        right_basis = orthonormal(matmul(cross_gram.T, left_basis))
        left_basis = orthonormal(matmul(cross_gram, right_basis))
    return (left_basis, right_basis)

def apply_stencil(field, conduct):
    padded = jnp.pad(field, ((1, 1), (1, 1), (1, 1), (0, 0)))
    center = padded[1:-1, 1:-1, 1:-1]
    beside = padded[2:, 1:-1, 1:-1] + padded[:-2, 1:-1, 1:-1]
    beside = beside + padded[1:-1, 2:, 1:-1] + padded[1:-1, :-2, 1:-1]
    beside = beside + padded[1:-1, 1:-1, 2:] + padded[1:-1, 1:-1, :-2]
    return conduct[..., None] * (beside - 6.0 * center) / 6.0

def reference(factor_obs, factor_ctrl, diffusivity, input_map, output_map, start_block, order):
    cell_count = NZ * NY * NX
    observe = factor_obs.reshape(cell_count, RANK)
    control = factor_ctrl.reshape(cell_count, RANK)
    cross_gram = matmul(observe.T, control)
    left_basis, right_basis = subspace_bases(cross_gram, start_block)
    ctrl_space = matmul(control, right_basis)
    obs_space = matmul(observe, left_basis)
    conduct = diffusivity.reshape(NZ, NY, NX)
    applied = apply_stencil(ctrl_space.reshape(NZ, NY, NX, RMAX), conduct).reshape(cell_count, RMAX)
    kept_mask = (jnp.arange(RMAX, dtype=jnp.int32) < order[0]).astype(jnp.float32)
    square_mask = kept_mask[:, None] * kept_mask[None, :]
    reduced_mass = square_mask * matmul(left_basis.T, matmul(cross_gram, right_basis))
    reduced_state = square_mask * matmul(obs_space.T, applied)
    drive = input_map.reshape(NIN, cell_count)
    sense = output_map.reshape(NOUT, cell_count)
    reduced_input = kept_mask[:, None] * matmul(drive, obs_space).T
    reduced_output = kept_mask[None, :] * matmul(sense, ctrl_space)
    return (reduced_mass, reduced_state, reduced_input, reduced_output)
```

```python
import functools
import jax
import jax.numpy as jnp
from jax import lax
from jax.experimental import pallas as pl
from jax.experimental.pallas import tpu as pltpu
from jax.sharding import PartitionSpec as P

LANES = 128
PANEL = 8
HIGHEST = lax.Precision.HIGHEST
HIGH = lax.Precision.HIGH


def exact(first, second, dims=((1,), (0,))):
    return lax.dot_general(
        first, second, (dims, ((), ())), precision=HIGHEST, preferred_element_type=jnp.float32
    )


def tall(first, second, dims=((1,), (0,))):
    return lax.dot_general(
        first, second, (dims, ((), ())), precision=HIGH, preferred_element_type=jnp.float32
    )


def sub_bits(count):
    return [1 << b for b in range(count.bit_length() - 1)]


def all_reduce_kernel(nslab, nsub, in_ref, out_ref, work, got_sub, got_slab, *sems):
    rs_sub_send, rs_sub_recv, rs_slab_send, rs_slab_recv = sems[:4]
    ag_slab_send, ag_slab_recv, ag_sub_send, ag_sub_recv = sems[4:]
    slab, sub = lax.axis_index("slab"), lax.axis_index("sub")
    rows, cols = work.shape[0], in_ref.shape[1]
    bits = sub_bits(nsub)

    def partner(bit):
        has = lax.rem(sub // bit, 2)
        return has, sub + bit - 2 * bit * has

    barrier = pltpu.get_barrier_semaphore()
    for bit in bits:
        pl.semaphore_signal(barrier, inc=1, device_id={"sub": partner(bit)[1]})
    for off in range(1, nslab):
        pl.semaphore_signal(barrier, inc=1, device_id={"slab": lax.rem(slab + off, nslab)})

    tall_rows = in_ref.shape[0]
    for c in range(cols // LANES):
        work[c * tall_rows : (c + 1) * tall_rows, :] = in_ref[:, c * LANES : (c + 1) * LANES]
    pl.semaphore_wait(barrier, len(bits) + nslab - 1)

    base, length, taken = 0, rows, 0
    for s, bit in enumerate(bits):
        half = length // 2
        has, other = partner(bit)
        keep = pl.multiple_of(base + has * half, 8)
        give = pl.multiple_of(base + (1 - has) * half, 8)
        copy = pltpu.make_async_remote_copy(
            src_ref=work.at[pl.ds(give, half)],
            dst_ref=got_sub.at[pl.ds(taken, half)],
            send_sem=rs_sub_send.at[s],
            recv_sem=rs_sub_recv.at[s],
            device_id={"sub": other},
        )
        copy.start()
        copy.wait()
        work[pl.ds(keep, half), :] += got_sub[taken : taken + half, :]
        base, length, taken = keep, half, taken + half

    piece = length // nslab
    copies = []
    for off in range(1, nslab):
        peer = lax.rem(slab + off, nslab)
        copy = pltpu.make_async_remote_copy(
            src_ref=work.at[pl.ds(pl.multiple_of(base + peer * piece, 8), piece)],
            dst_ref=got_slab.at[off],
            send_sem=rs_slab_send.at[off],
            recv_sem=rs_slab_recv.at[off],
            device_id={"slab": peer},
        )
        copy.start()
        copies.append(copy)
    mine = pl.multiple_of(base + slab * piece, 8)
    total = work[pl.ds(mine, piece), :]
    for off in range(1, nslab):
        copies[off - 1].wait_recv()
        total = total + got_slab[off]
    out_ref[pl.ds(mine, piece), :] = total
    for copy in copies:
        copy.wait_send()

    copies = []
    for off in range(1, nslab):
        copy = pltpu.make_async_remote_copy(
            src_ref=out_ref.at[pl.ds(mine, piece)],
            dst_ref=out_ref.at[pl.ds(mine, piece)],
            send_sem=ag_slab_send.at[off],
            recv_sem=ag_slab_recv.at[off],
            device_id={"slab": lax.rem(slab + off, nslab)},
        )
        copy.start()
        copies.append(copy)
    for copy in copies:
        copy.wait()

    for s in reversed(range(len(bits))):
        has, other = partner(bits[s])
        copy = pltpu.make_async_remote_copy(
            src_ref=out_ref.at[pl.ds(base, length)],
            dst_ref=out_ref.at[pl.ds(base, length)],
            send_sem=ag_sub_send.at[s],
            recv_sem=ag_sub_recv.at[s],
            device_id={"sub": other},
        )
        copy.start()
        copy.wait()
        base = pl.multiple_of(base - has * length, 8)
        length = 2 * length


def all_reduce(part, ident):
    nslab, nsub = lax.axis_size("slab"), lax.axis_size("sub")
    rows = part.shape[0] * (part.shape[1] // LANES)
    bits = len(sub_bits(nsub))
    piece = rows // (nsub * nslab)
    sub_sem, slab_sem = pltpu.SemaphoreType.DMA((bits,)), pltpu.SemaphoreType.DMA((nslab,))
    return pl.pallas_call(
        functools.partial(all_reduce_kernel, nslab, nsub),
        out_shape=jax.ShapeDtypeStruct((rows, LANES), jnp.float32),
        in_specs=[pl.BlockSpec(memory_space=pltpu.VMEM)],
        out_specs=pl.BlockSpec(memory_space=pltpu.VMEM),
        scratch_shapes=[
            pltpu.VMEM((rows, LANES), jnp.float32),
            pltpu.VMEM((rows, LANES), jnp.float32),
            pltpu.VMEM((nslab, piece, LANES), jnp.float32),
            sub_sem, sub_sem, slab_sem, slab_sem, slab_sem, slab_sem, sub_sem, sub_sem,
        ],
        compiler_params=pltpu.CompilerParams(collective_id=ident, has_side_effects=True),
    )(part)


def inverse_factor(work, size):
    for base in range(0, size, PANEL):
        rows = [
            jnp.broadcast_to(work[base + i : base + i + 1, :], (PANEL, 2 * size))
            for i in range(PANEL)
        ]
        block = [
            [
                jnp.broadcast_to(rows[i][:, base + j : base + j + 1], (PANEL, LANES))
                if j >= i
                else None
                for j in range(PANEL)
            ]
            for i in range(PANEL)
        ]
        wide = 2 * size // LANES
        for j in range(PANEL):
            scale = lax.rsqrt(block[j][j])
            lead = [block[j][i] * scale if i > j else None for i in range(PANEL)]
            rows[j] = rows[j] * jnp.concatenate([scale] * wide, axis=1)
            for i in range(j + 1, PANEL):
                for m in range(i, PANEL):
                    block[i][m] = block[i][m] - lead[i] * lead[m]
                rows[i] = rows[i] - jnp.concatenate([lead[i]] * wide, axis=1) * rows[j]
        place = lax.broadcasted_iota(jnp.int32, (PANEL, 2 * size), 0)
        panel = rows[0]
        for i in range(1, PANEL):
            panel = jnp.where(place == i, rows[i], panel)
        work[base : base + PANEL, :] = panel
        if base + PANEL < size:
            left = panel[:, :size]
            update = exact(left, panel, ((0,), (0,)))
            work[base + PANEL :, :] = work[base + PANEL :, :] - update[base + PANEL :, :]


def bases_kernel(sweeps, gram_ref, start_ref, left_ref, right_ref, mass_ref, both, block, work):
    rank, size = start_ref.shape
    for c in range(rank // LANES):
        cols = slice(c * LANES, (c + 1) * LANES)
        tile = gram_ref[c * rank : (c + 1) * rank, :]
        both[1, :, cols] = tile
        both[0, cols, :] = tile.T
    block[...] = start_ref[...]
    row = lax.broadcasted_iota(jnp.int32, (size, size), 0)
    col = lax.broadcasted_iota(jnp.int32, (size, size), 1)
    eye = (row == col).astype(jnp.float32)

    def step(k, carry):
        product = exact(both[lax.rem(k, 2)], block[...])
        work[:, :size] = exact(product, product, ((0,), (0,)))
        work[:, size:] = eye
        inverse_factor(work, size)
        right_ref[...] = left_ref[...]
        basis = exact(product, work[:, size:], ((1,), (1,)))
        block[...] = basis
        left_ref[...] = basis
        return carry

    left_ref[...] = start_ref[...]
    lax.fori_loop(0, 2 * sweeps, step, 0)
    mass_ref[...] = exact(left_ref[...], exact(both[1], right_ref[...]), ((0,), (0,)))


def subspace_bases(cross_gram, start_block):
    rank, size = start_block.shape
    tall_shape = jax.ShapeDtypeStruct((rank, size), jnp.float32)
    vmem = pl.BlockSpec(memory_space=pltpu.VMEM)
    return pl.pallas_call(
        functools.partial(bases_kernel, 2),
        out_shape=(tall_shape, tall_shape, jax.ShapeDtypeStruct((size, size), jnp.float32)),
        in_specs=[vmem, vmem],
        out_specs=(vmem, vmem, vmem),
        scratch_shapes=[
            pltpu.VMEM((2, rank, rank), jnp.float32),
            pltpu.VMEM((rank, size), jnp.float32),
            pltpu.VMEM((size, 2 * size), jnp.float32),
        ],
    )(cross_gram, start_block)


def shifted(face, axis, step):
    count = lax.axis_size(axis)
    pairs = [(i, i + step) for i in range(count) if 0 <= i + step < count]
    return lax.ppermute(face, axis, pairs)


def on_device(factor_obs, factor_ctrl, diffusivity, input_map, output_map, start_block, order):
    planes, lines, points, rank = factor_ctrl.shape
    cells = planes * lines * points
    size = start_block.shape[1]
    observe = factor_obs.reshape(cells, rank)
    control = factor_ctrl.reshape(cells, rank)
    conduct = diffusivity.reshape(planes, lines, points)
    drive = input_map.reshape(input_map.shape[0], cells)
    sense = output_map.reshape(output_map.shape[0], cells)
    ins, outs = drive.shape[0], sense.shape[0]

    cross_gram = all_reduce(tall(observe, control, ((0,), (0,))), 0)
    left_basis, right_basis, mass = subspace_bases(cross_gram, start_block)

    ctrl_flat = tall(control, right_basis)
    ctrl = ctrl_flat.reshape(planes, lines, points, size)
    below = shifted(ctrl[-1:], "slab", 1)
    above = shifted(ctrl[:1], "slab", -1)
    before = shifted(ctrl[:, -1:], "sub", 1)
    after = shifted(ctrl[:, :1], "sub", -1)
    obs_space = tall(observe, left_basis)
    zs = jnp.concatenate([below, ctrl, above], axis=0)
    ys = jnp.concatenate([before, ctrl, after], axis=1)
    xs = jnp.pad(ctrl, ((0, 0), (0, 0), (1, 1), (0, 0)))
    beside = zs[2:] + zs[:-2] + ys[:, 2:] + ys[:, :-2] + xs[:, :, 2:] + xs[:, :, :-2]
    applied = (conduct[..., None] * (beside - 6.0 * ctrl) / 6.0).reshape(cells, size)
    state = tall(obs_space, applied, ((0,), (0,)))
    used = size + ins + outs
    grain = 8 * lax.axis_size("slab") * lax.axis_size("sub")
    packed = jnp.concatenate(
        [
            state,
            tall(drive, obs_space),
            tall(sense, ctrl_flat),
            jnp.zeros((-used % grain, size), jnp.float32),
        ],
        axis=0,
    )
    summed = all_reduce(packed, 1)
    kept = (jnp.arange(size, dtype=jnp.int32) < order[0]).astype(jnp.float32)
    square = kept[:, None] * kept[None, :]
    reduced_input = kept[:, None] * summed[size : size + ins].T
    reduced_output = kept[None, :] * summed[size + ins : used]
    return (square * mass, square * summed[:size], reduced_input, reduced_output)


def solution(mesh):
    placed = (
        P("slab", "sub", None, None),
        P("slab", "sub", None, None),
        P("slab", "sub"),
        P(None, "slab", "sub"),
        P(None, "slab", "sub"),
        P(),
        P(),
    )
    return jax.shard_map(
        on_device, mesh=mesh, in_specs=placed, out_specs=(P(), P(), P(), P()), check_vma=False
    )
```

```python
import functools
import jax
import jax.numpy as jnp
from jax import lax
from jax.experimental import pallas as pl
from jax.experimental.pallas import tpu as pltpu
from jax.sharding import PartitionSpec as P

LANES = 128
PANEL = 8
HIGHEST = lax.Precision.HIGHEST
HIGH = lax.Precision.HIGH


def exact(first, second, dims=((1,), (0,))):
    return lax.dot_general(
        first, second, (dims, ((), ())), precision=HIGHEST, preferred_element_type=jnp.float32
    )


def tall(first, second, dims=((1,), (0,))):
    return lax.dot_general(
        first, second, (dims, ((), ())), precision=HIGH, preferred_element_type=jnp.float32
    )


def narrow(first, second, dims=((1,), (0,))):
    return lax.dot_general(first, second, (dims, ((), ())), preferred_element_type=jnp.float32)


def three_parts(value):
    high = value.astype(jnp.bfloat16).astype(jnp.float32)
    mid = (value - high).astype(jnp.bfloat16).astype(jnp.float32)
    return high, mid, value - high - mid


def two_parts(value):
    high = value.astype(jnp.bfloat16)
    return high, (value - high.astype(jnp.float32)).astype(jnp.bfloat16)


def three_dots(first, second, dims=((1,), (0,))):
    (a, b), (c, d) = two_parts(first), two_parts(second)
    return narrow(a, c, dims) + (narrow(a, d, dims) + narrow(b, c, dims))


def gram_kernel(first_ref, second_ref, out_ref):
    @pl.when(pl.program_id(0) == 0)
    def _():
        out_ref[...] = jnp.zeros_like(out_ref)

    out_ref[...] += three_dots(first_ref[...], second_ref[...], ((0,), (0,)))


def cells_step(cells):
    return 512 if cells % 512 == 0 else cells


def gram(first, second):
    cells, wide = first.shape
    step = cells_step(cells)
    spec = pl.BlockSpec((step, wide), lambda k: (k, 0))
    return pl.pallas_call(
        gram_kernel,
        grid=(cells // step,),
        out_shape=jax.ShapeDtypeStruct((wide, second.shape[1]), jnp.float32),
        in_specs=[spec, spec],
        out_specs=pl.BlockSpec((wide, second.shape[1]), lambda k: (0, 0)),
        compiler_params=pltpu.CompilerParams(dimension_semantics=("arbitrary",)),
    )(first, second)


def sub_bits(count):
    return [1 << b for b in range(count.bit_length() - 1)]


def all_reduce_kernel(nslab, nsub, in_ref, out_ref, work, got_sub, got_slab, *sems):
    rs_sub_send, rs_sub_recv, rs_slab_send, rs_slab_recv = sems[:4]
    ag_slab_send, ag_slab_recv, ag_sub_send, ag_sub_recv = sems[4:]
    slab, sub = lax.axis_index("slab"), lax.axis_index("sub")
    rows, cols = work.shape[0], in_ref.shape[1]
    bits = sub_bits(nsub)

    def partner(bit):
        has = lax.rem(sub // bit, 2)
        return has, sub + bit - 2 * bit * has

    barrier = pltpu.get_barrier_semaphore()
    for bit in bits:
        pl.semaphore_signal(barrier, inc=1, device_id={"sub": partner(bit)[1]})
    for off in range(1, nslab):
        pl.semaphore_signal(barrier, inc=1, device_id={"slab": lax.rem(slab + off, nslab)})

    tall_rows = in_ref.shape[0]
    for c in range(cols // LANES):
        work[c * tall_rows : (c + 1) * tall_rows, :] = in_ref[:, c * LANES : (c + 1) * LANES]
    pl.semaphore_wait(barrier, len(bits) + nslab - 1)

    base, length, taken = 0, rows, 0
    for s, bit in enumerate(bits):
        half = length // 2
        has, other = partner(bit)
        keep = pl.multiple_of(base + has * half, 8)
        give = pl.multiple_of(base + (1 - has) * half, 8)
        copy = pltpu.make_async_remote_copy(
            src_ref=work.at[pl.ds(give, half)],
            dst_ref=got_sub.at[pl.ds(taken, half)],
            send_sem=rs_sub_send.at[s],
            recv_sem=rs_sub_recv.at[s],
            device_id={"sub": other},
        )
        copy.start()
        copy.wait()
        work[pl.ds(keep, half), :] += got_sub[taken : taken + half, :]
        base, length, taken = keep, half, taken + half

    piece = length // nslab
    copies = []
    for off in range(1, nslab):
        peer = lax.rem(slab + off, nslab)
        copy = pltpu.make_async_remote_copy(
            src_ref=work.at[pl.ds(pl.multiple_of(base + peer * piece, 8), piece)],
            dst_ref=got_slab.at[off],
            send_sem=rs_slab_send.at[off],
            recv_sem=rs_slab_recv.at[off],
            device_id={"slab": peer},
        )
        copy.start()
        copies.append(copy)
    mine = pl.multiple_of(base + slab * piece, 8)
    total = work[pl.ds(mine, piece), :]
    for off in range(1, nslab):
        copies[off - 1].wait_recv()
        total = total + got_slab[off]
    out_ref[pl.ds(mine, piece), :] = total
    for copy in copies:
        copy.wait_send()

    copies = []
    for off in range(1, nslab):
        copy = pltpu.make_async_remote_copy(
            src_ref=out_ref.at[pl.ds(mine, piece)],
            dst_ref=out_ref.at[pl.ds(mine, piece)],
            send_sem=ag_slab_send.at[off],
            recv_sem=ag_slab_recv.at[off],
            device_id={"slab": lax.rem(slab + off, nslab)},
        )
        copy.start()
        copies.append(copy)
    for copy in copies:
        copy.wait()

    for s in reversed(range(len(bits))):
        has, other = partner(bits[s])
        copy = pltpu.make_async_remote_copy(
            src_ref=out_ref.at[pl.ds(base, length)],
            dst_ref=out_ref.at[pl.ds(base, length)],
            send_sem=ag_sub_send.at[s],
            recv_sem=ag_sub_recv.at[s],
            device_id={"sub": other},
        )
        copy.start()
        copy.wait()
        base = pl.multiple_of(base - has * length, 8)
        length = 2 * length


def all_reduce(part, ident):
    nslab, nsub = lax.axis_size("slab"), lax.axis_size("sub")
    rows = part.shape[0] * (part.shape[1] // LANES)
    bits = len(sub_bits(nsub))
    piece = rows // (nsub * nslab)
    sub_sem, slab_sem = pltpu.SemaphoreType.DMA((bits,)), pltpu.SemaphoreType.DMA((nslab,))
    return pl.pallas_call(
        functools.partial(all_reduce_kernel, nslab, nsub),
        out_shape=jax.ShapeDtypeStruct((rows, LANES), jnp.float32),
        in_specs=[pl.BlockSpec(memory_space=pltpu.VMEM)],
        out_specs=pl.BlockSpec(memory_space=pltpu.VMEM),
        scratch_shapes=[
            pltpu.VMEM((rows, LANES), jnp.float32),
            pltpu.VMEM((rows, LANES), jnp.float32),
            pltpu.VMEM((nslab, piece, LANES), jnp.float32),
            sub_sem, sub_sem, slab_sem, slab_sem, slab_sem, slab_sem, sub_sem, sub_sem,
        ],
        compiler_params=pltpu.CompilerParams(collective_id=ident, has_side_effects=True),
    )(part)


def small_kernel(nslab, nsub, in_ref, out_ref, total, slots, got_slab, *sems):
    sub_send, sub_recv, rs_send, rs_recv, ag_send, ag_recv = sems
    slab, sub = lax.axis_index("slab"), lax.axis_index("sub")
    barrier = pltpu.get_barrier_semaphore()
    for off in range(1, nsub):
        pl.semaphore_signal(barrier, inc=1, device_id={"sub": lax.rem(sub + off, nsub)})
    for off in range(1, nslab):
        pl.semaphore_signal(barrier, inc=1, device_id={"slab": lax.rem(slab + off, nslab)})
    pl.semaphore_wait(barrier, nsub + nslab - 2)

    copies = []
    for off in range(1, nsub):
        copy = pltpu.make_async_remote_copy(
            src_ref=in_ref,
            dst_ref=slots.at[sub],
            send_sem=sub_send.at[off],
            recv_sem=sub_recv.at[off],
            device_id={"sub": lax.rem(sub + off, nsub)},
        )
        copy.start()
        copies.append(copy)
    slots[sub] = in_ref[...]
    for copy in copies:
        copy.wait()
    value = slots[0]
    for k in range(1, nsub):
        value = value + slots[k]
    total[...] = value

    piece = in_ref.shape[0] // nslab
    copies = []
    for off in range(1, nslab):
        peer = lax.rem(slab + off, nslab)
        copy = pltpu.make_async_remote_copy(
            src_ref=total.at[pl.ds(pl.multiple_of(peer * piece, 8), piece)],
            dst_ref=got_slab.at[off],
            send_sem=rs_send.at[off],
            recv_sem=rs_recv.at[off],
            device_id={"slab": peer},
        )
        copy.start()
        copies.append(copy)
    mine = pl.multiple_of(slab * piece, 8)
    value = total[pl.ds(mine, piece), :]
    for off in range(1, nslab):
        copies[off - 1].wait()
        value = value + got_slab[off]
    out_ref[pl.ds(mine, piece), :] = value
    copies = []
    for off in range(1, nslab):
        copy = pltpu.make_async_remote_copy(
            src_ref=out_ref.at[pl.ds(mine, piece)],
            dst_ref=out_ref.at[pl.ds(mine, piece)],
            send_sem=ag_send.at[off],
            recv_sem=ag_recv.at[off],
            device_id={"slab": lax.rem(slab + off, nslab)},
        )
        copy.start()
        copies.append(copy)
    for copy in copies:
        copy.wait()


def small_all_reduce(part, ident):
    nslab, nsub = lax.axis_size("slab"), lax.axis_size("sub")
    rows = part.shape[0]
    sub_sem, slab_sem = pltpu.SemaphoreType.DMA((nsub,)), pltpu.SemaphoreType.DMA((nslab,))
    return pl.pallas_call(
        functools.partial(small_kernel, nslab, nsub),
        out_shape=jax.ShapeDtypeStruct((rows, LANES), jnp.float32),
        in_specs=[pl.BlockSpec(memory_space=pltpu.VMEM)],
        out_specs=pl.BlockSpec(memory_space=pltpu.VMEM),
        scratch_shapes=[
            pltpu.VMEM((rows, LANES), jnp.float32),
            pltpu.VMEM((nsub, rows, LANES), jnp.float32),
            pltpu.VMEM((nslab, rows // nslab, LANES), jnp.float32),
            sub_sem, sub_sem, slab_sem, slab_sem, slab_sem, slab_sem,
        ],
        compiler_params=pltpu.CompilerParams(collective_id=ident, has_side_effects=True),
    )(part)


def inverse_factor(work, size):
    for base in range(0, size, PANEL):
        rows = [
            jnp.broadcast_to(work[base + i : base + i + 1, :], (PANEL, 2 * size))
            for i in range(PANEL)
        ]
        block = [
            [
                jnp.broadcast_to(rows[i][:, base + j : base + j + 1], (PANEL, LANES))
                if j >= i
                else None
                for j in range(PANEL)
            ]
            for i in range(PANEL)
        ]
        wide = 2 * size // LANES
        for j in range(PANEL):
            scale = lax.rsqrt(block[j][j])
            lead = [block[j][i] * scale if i > j else None for i in range(PANEL)]
            rows[j] = rows[j] * jnp.concatenate([scale] * wide, axis=1)
            for i in range(j + 1, PANEL):
                for m in range(i, PANEL):
                    block[i][m] = block[i][m] - lead[i] * lead[m]
                rows[i] = rows[i] - jnp.concatenate([lead[i]] * wide, axis=1) * rows[j]
        place = lax.broadcasted_iota(jnp.int32, (PANEL, 2 * size), 0)
        panel = rows[0]
        for i in range(1, PANEL):
            panel = jnp.where(place == i, rows[i], panel)
        work[base : base + PANEL, :] = panel
        if base + PANEL < size:
            high, mid, low = three_parts(panel)
            first = jnp.concatenate([high, high, mid, high, low, mid], axis=0)[:, :size]
            second = jnp.concatenate([high, mid, high, low, high, mid], axis=0)
            update = narrow(first.astype(jnp.bfloat16), second.astype(jnp.bfloat16), ((0,), (0,)))
            work[base + PANEL :, :] = work[base + PANEL :, :] - update[base + PANEL :, :]


def bases_kernel(sweeps, gram_ref, start_ref, left_ref, right_ref, mass_ref, both, block, work):
    rank, size = start_ref.shape
    for c in range(rank // LANES):
        cols = slice(c * LANES, (c + 1) * LANES)
        tile = gram_ref[c * rank : (c + 1) * rank, :]
        both[1, :, cols] = tile
        both[0, cols, :] = tile.T
    block[...] = start_ref[...]
    row = lax.broadcasted_iota(jnp.int32, (size, size), 0)
    col = lax.broadcasted_iota(jnp.int32, (size, size), 1)
    eye = (row == col).astype(jnp.float32)

    def step(k, carry):
        product = exact(both[lax.rem(k, 2)], block[...])
        work[:, :size] = exact(product, product, ((0,), (0,)))
        work[:, size:] = eye
        inverse_factor(work, size)
        right_ref[...] = left_ref[...]
        basis = exact(product, work[:, size:], ((1,), (1,)))
        block[...] = basis
        left_ref[...] = basis
        return carry

    left_ref[...] = start_ref[...]
    lax.fori_loop(0, 2 * sweeps, step, 0)
    mass_ref[...] = exact(left_ref[...], exact(both[1], right_ref[...]), ((0,), (0,)))


def subspace_bases(cross_gram, start_block):
    rank, size = start_block.shape
    tall_shape = jax.ShapeDtypeStruct((rank, size), jnp.float32)
    vmem = pl.BlockSpec(memory_space=pltpu.VMEM)
    return pl.pallas_call(
        functools.partial(bases_kernel, 2),
        out_shape=(tall_shape, tall_shape, jax.ShapeDtypeStruct((size, size), jnp.float32)),
        in_specs=[vmem, vmem],
        out_specs=(vmem, vmem, vmem),
        scratch_shapes=[
            pltpu.VMEM((2, rank, rank), jnp.float32),
            pltpu.VMEM((rank, size), jnp.float32),
            pltpu.VMEM((size, 2 * size), jnp.float32),
        ],
    )(cross_gram, start_block)


def block_order(k, count, per_plane):
    inner = jnp.where(k < 2 * per_plane, count - 2 * per_plane + k, k - per_plane)
    return jnp.where(k < per_plane, k, inner)


def project_kernel(nslab, nsub, per_plane, *refs):
    ctrl_cells, obs_cells, right_ref, left_ref, ctrl_ref, obs_ref = refs[:6]
    faces, halves, landed, (send, recv) = refs[6:10], refs[10], refs[11:15], refs[15:]
    k = pl.program_id(0)
    count = pl.num_programs(0) // 2
    planes, lines, points, size = ctrl_ref.shape
    slab, sub = lax.axis_index("slab"), lax.axis_index("sub")
    moves = (
        ("slab", slab, nslab, 1, ctrl_ref.at[planes - 1]),
        ("slab", slab, nslab, -1, ctrl_ref.at[0]),
        ("sub", sub, nsub, 1, ctrl_ref.at[:, lines - 1]),
        ("sub", sub, nsub, -1, ctrl_ref.at[:, 0]),
    )

    def there(me, total, step):
        return me < total - 1 if step > 0 else me > 0

    def copy(m):
        axis, me, _, step, source = moves[m]
        return pltpu.make_async_remote_copy(
            src_ref=source,
            dst_ref=landed[m],
            send_sem=send.at[m],
            recv_sem=recv.at[m],
            device_id={axis: me + step},
        )

    def each(picked, act):
        for m in picked:
            _, me, total, step, _ = moves[m]

            @pl.when(there(me, total, step))
            def _():
                act(m)

    def product(cells, which):
        high, low = two_parts(cells)
        wide = narrow(high, halves[which])
        return wide[:, :size] + (wide[:, size:] + narrow(low, halves[which, :, :size]))

    @pl.when(k == 0)
    def _():
        barrier = pltpu.get_barrier_semaphore()
        for axis, me, total, step, _ in moves:
            beside = lax.rem(me + step + total, total)
            pl.semaphore_signal(barrier, inc=1, device_id={axis: beside})
        pl.semaphore_wait(barrier, len(moves))
        for which, basis in enumerate((right_ref, left_ref)):
            high, low = two_parts(basis[...])
            halves[which, :, :size] = high
            halves[which, :, size:] = low

    @pl.when(k < count)
    def _():
        block = block_order(k, count, per_plane)
        some = lines // per_plane
        value = product(ctrl_cells[...], 0).reshape(some, points, size)
        ctrl_ref[block // per_plane, pl.ds(lax.rem(block, per_plane) * some, some)] = value

    @pl.when(k >= count)
    def _():
        obs_ref[...] = product(obs_cells[...], 1)

    @pl.when(k == 2 * per_plane - 1)
    def _():
        each((0, 1), lambda m: copy(m).start())

    @pl.when(k == count - 1)
    def _():
        each((2, 3), lambda m: copy(m).start())

    @pl.when(k == 2 * count - 1)
    def _():
        for m, (_, me, total, step, _) in enumerate(moves):

            @pl.when(there(me, total, step))
            def _():
                copy(m).wait_send()

            @pl.when(there(me, total, -step))
            def _():
                copy(m).wait_recv()
                faces[m][...] = landed[m][...]

            @pl.when(jnp.logical_not(there(me, total, -step)))
            def _():
                faces[m][...] = jnp.zeros(landed[m].shape, jnp.float32)


def project(factor_ctrl, factor_obs, right_basis, left_basis, ident):
    nslab, nsub = lax.axis_size("slab"), lax.axis_size("sub")
    planes, lines, points, wide = factor_ctrl.shape
    cells, size = planes * lines * points, right_basis.shape[1]
    per_plane = 2 if lines % 2 == 0 else 1
    count, step = planes * per_plane, lines * points // per_plane
    shapes = [(lines, points, size)] * 2 + [(planes, points, size)] * 2
    grid_shape = (planes, lines, points, size)
    four = pltpu.SemaphoreType.DMA((4,))
    basis_spec = pl.BlockSpec((wide, size), lambda k: (0, 0))
    return pl.pallas_call(
        functools.partial(project_kernel, nslab, nsub, per_plane),
        grid=(2 * count,),
        out_shape=[
            jax.ShapeDtypeStruct(grid_shape, jnp.float32),
            jax.ShapeDtypeStruct((cells, size), jnp.float32),
        ]
        + [jax.ShapeDtypeStruct(shape, jnp.float32) for shape in shapes],
        in_specs=[
            pl.BlockSpec(
                (step, wide),
                lambda k: (block_order(jnp.minimum(k, count - 1), count, per_plane), 0),
            ),
            pl.BlockSpec((step, wide), lambda k: (jnp.maximum(k - count, 0), 0)),
            basis_spec,
            basis_spec,
        ],
        out_specs=[
            pl.BlockSpec(grid_shape, lambda k: (0, 0, 0, 0)),
            pl.BlockSpec((step, size), lambda k: (jnp.maximum(k - count, 0), 0)),
        ]
        + [pl.BlockSpec(shape, lambda k: (0, 0, 0)) for shape in shapes],
        scratch_shapes=[pltpu.VMEM((2, wide, 2 * size), jnp.bfloat16)]
        + [pltpu.VMEM(shape, jnp.float32) for shape in shapes]
        + [four, four],
        compiler_params=pltpu.CompilerParams(
            collective_id=ident,
            has_side_effects=True,
            dimension_semantics=("arbitrary",),
        ),
    )(factor_ctrl.reshape(cells, wide), factor_obs.reshape(cells, wide), right_basis, left_basis)


def on_device(factor_obs, factor_ctrl, diffusivity, input_map, output_map, start_block, order):
    planes, lines, points, rank = factor_ctrl.shape
    cells = planes * lines * points
    size = start_block.shape[1]
    observe = factor_obs.reshape(cells, rank)
    control = factor_ctrl.reshape(cells, rank)
    conduct = diffusivity.reshape(planes, lines, points)
    drive = input_map.reshape(input_map.shape[0], cells)
    sense = output_map.reshape(output_map.shape[0], cells)
    ins, outs = drive.shape[0], sense.shape[0]

    cross_gram = all_reduce(gram(observe, control), 0)
    left_basis, right_basis, mass = subspace_bases(cross_gram, start_block)

    ctrl, obs_space, below, above, before, after = project(
        factor_ctrl, factor_obs, right_basis, left_basis, 2
    )
    ctrl_flat = ctrl.reshape(cells, size)
    below, above = below[None], above[None]
    before, after = before[:, None], after[:, None]
    zs = jnp.concatenate([below, ctrl, above], axis=0)
    ys = jnp.concatenate([before, ctrl, after], axis=1)
    xs = jnp.pad(ctrl, ((0, 0), (0, 0), (1, 1), (0, 0)))
    beside = zs[2:] + zs[:-2] + ys[:, 2:] + ys[:, :-2] + xs[:, :, 2:] + xs[:, :, :-2]
    applied = (conduct[..., None] * (beside - 6.0 * ctrl) / 6.0).reshape(cells, size)
    state = tall(obs_space, applied, ((0,), (0,)))
    used = size + ins + outs
    grain = 8 * lax.axis_size("slab")
    packed = jnp.concatenate(
        [
            state,
            tall(drive, obs_space),
            tall(sense, ctrl_flat),
            jnp.zeros((-used % grain, size), jnp.float32),
        ],
        axis=0,
    )
    summed = small_all_reduce(packed, 1)
    kept = (jnp.arange(size, dtype=jnp.int32) < order[0]).astype(jnp.float32)
    square = kept[:, None] * kept[None, :]
    reduced_input = kept[:, None] * summed[size : size + ins].T
    reduced_output = kept[None, :] * summed[size + ins : used]
    return (square * mass, square * summed[:size], reduced_input, reduced_output)


def solution(mesh):
    placed = (
        P("slab", "sub", None, None),
        P("slab", "sub", None, None),
        P("slab", "sub"),
        P(None, "slab", "sub"),
        P(None, "slab", "sub"),
        P(),
        P(),
    )
    return jax.shard_map(
        on_device, mesh=mesh, in_specs=placed, out_specs=(P(), P(), P(), P()), check_vma=False
    )
```
